128 devices in a mesh: rep: 8 (over y, z_lo), tp: 16 (over x, z_hi, core).
Axes of the slice: x: 4, y: 4, z: 4 (z_hi: 2, z_lo: 2; z = z_hi * 2 + z_lo), core: 2. Of those that a mesh axis runs over, the one named last changes fastest.
Arguments:
- deltas: bfloat16 [8, 3, 4096, 8192], P('rep', None, 'tp'), may hold values from -2600 to 2600
- staleness: int32 [8], P('rep'), may hold values from 0 to 2
Outputs:
- update: bfloat16 [4096, 8192], P('tp')
The draws below stay inside these ranges and needn't reach their ends.
All inputs are finite; a program needn't handle non-finite values.
Results may differ from the reference program's by a relative error of at most 0.028.
Values may be sent and summed in bfloat16 or wider, within the bound.
No kernel may reach another device: no remote copies, remote signals or barrier semaphores. Data moves between devices by JAX's collectives and lax.ppermute only.
A program may use at most 128 MiB of HBM per device.

```python
import jax
import jax.numpy as jnp
from jax import lax

ROWS = 4096
COLS = 8192
TILE = 512
SNAPS = 3
NS_ITERS = 5
REPLICAS = 8
N_REP = 8


def draw_deltas(key, part):
    keys = jax.random.split(key, 3)
    base = jax.random.truncated_normal(keys[0], -6.0, 6.0, (REPLICAS, SNAPS, ROWS, COLS), jnp.float32)
    replica_scale = 3.0 ** (jnp.arange(REPLICAS, dtype=jnp.float32) / max(REPLICAS - 1, 1))
    row_scale = jax.random.uniform(keys[1], (ROWS,), jnp.float32, 0.5, 2.0)
    col_scale = jax.random.uniform(keys[2], (COLS,), jnp.float32, 0.5, 2.0)
    mixed = base
    values = mixed * row_scale[:, None] * col_scale[None, :] * replica_scale[:, None, None, None]
    return values.astype(jnp.bfloat16)


def place_ends(entries, own_key, smallest, high):
    dims = entries.shape
    index_at = [jax.random.randint(jax.random.fold_in(own_key, axis), (), 0, dims[axis]) for axis in range(len(dims))]
    entries = entries.at[tuple(index_at)].set(smallest)
    longest = dims.index(max(dims))
    index_at[longest] = (index_at[longest] + 1) % dims[longest]
    return entries.at[tuple(index_at)].set(high)


def setup_inputs(seed: int = 0) -> dict:
    seeds = jax.random.split(jax.random.key(seed), 3)
    return {
        "deltas": draw_deltas(jax.random.fold_in(seeds[2], 71), 0),
        "staleness": place_ends(jax.random.randint(seeds[1], (REPLICAS,), 0, SNAPS), jax.random.fold_in(seeds[1], 1), 0, SNAPS - 1).astype(jnp.int32),
    }


damping = 0.001

def newton_root(stat):
    identity = jnp.eye(TILE, dtype=jnp.float32)
    frob_norm = jnp.sqrt(jnp.sum(stat * stat))
    current = stat / frob_norm
    iterate = identity
    for step in range(NS_ITERS):
        factor = (5.0 * identity - current) * 0.25
        iterate = jnp.dot(iterate, factor, precision=lax.Precision.HIGHEST, preferred_element_type=jnp.float32)
        if step + 1 < NS_ITERS:
            square = jnp.dot(factor, factor, precision=lax.Precision.HIGHEST, preferred_element_type=jnp.float32)
            fourth = jnp.dot(square, square, precision=lax.Precision.HIGHEST, preferred_element_type=jnp.float32)
            current = jnp.dot(fourth, current, precision=lax.Precision.HIGHEST, preferred_element_type=jnp.float32)
    return (iterate * frob_norm ** (-0.25)).astype(jnp.bfloat16)

def reference(deltas, staleness):
    picked = deltas[jnp.arange(REPLICAS), staleness]
    mean_delta = (lax.optimization_barrier(jnp.sum(picked.astype(jnp.float32), axis=0)) / N_REP).astype(jnp.bfloat16)
    row_blocks = ROWS // TILE
    col_blocks = COLS // TILE
    identity = jnp.eye(TILE, dtype=jnp.float32)

    def tile_update(index):
        row_start = (index // col_blocks * TILE).astype(jnp.int32)
        col_start = (index % col_blocks * TILE).astype(jnp.int32)
        block = lax.dynamic_slice(picked, (jnp.int32(0), row_start, col_start), (REPLICAS, TILE, TILE)).astype(jnp.float32)
        left_gram = jnp.einsum('rij,rkj->ik', block, block, precision=lax.Precision.HIGHEST)
        right_gram = jnp.einsum('rji,rjk->ik', block, block, precision=lax.Precision.HIGHEST)
        left_root = newton_root(left_gram / (N_REP * TILE) + damping * identity)
        right_root = newton_root(right_gram / (N_REP * TILE) + damping * identity)
        mean_tile = lax.dynamic_slice(mean_delta, (row_start, col_start), (TILE, TILE))
        half_product = jnp.dot(left_root, mean_tile, preferred_element_type=jnp.float32).astype(jnp.bfloat16)
        return jnp.dot(half_product, right_root, preferred_element_type=jnp.float32).astype(jnp.bfloat16)
    tiles = lax.map(tile_update, jnp.arange(row_blocks * col_blocks, dtype=jnp.int32))
    return tiles.reshape(row_blocks, col_blocks, TILE, TILE).transpose(0, 2, 1, 3).reshape(ROWS, COLS)
```

```python
import jax
import jax.numpy as jnp
from jax import lax
from jax.sharding import Mesh, PartitionSpec as P

TILE = 512
NS_ITERS = 5
CORES = 2

damping = 0.001


def multiply(left_side, right_side):
    return jnp.einsum("xij,xjk->xik", left_side, right_side)


def inverse_roots(stat_stack):
    identity = jnp.eye(TILE, dtype=jnp.float32)
    frob_norm = jnp.sqrt(jnp.sum(stat_stack * stat_stack, axis=(1, 2), keepdims=True))
    current = stat_stack / frob_norm
    iterate = None
    for step in range(NS_ITERS):
        factor = (5.0 * identity - current) * 0.25
        iterate = factor if iterate is None else multiply(iterate, factor)
        if step + 1 < NS_ITERS:
            square = multiply(factor, factor)
            fourth = multiply(square, square)
            current = multiply(fourth, current)
    return (iterate * frob_norm ** (-0.25)).astype(jnp.bfloat16)


def local(deltas, staleness):
    replicas = lax.axis_size("rep")
    group = replicas * CORES
    picked = lax.dynamic_index_in_dim(deltas[0], staleness[0], 0, keepdims=False)
    rows = picked.shape[0]
    blocks = picked.reshape(rows, group, TILE).transpose(1, 0, 2)
    received = lax.all_to_all(blocks, ("rep", "core"), split_axis=0, concat_axis=0, tiled=True)
    tiles = received.reshape(replicas, TILE, TILE)
    left_gram = jnp.einsum("rik,rjk->ij", tiles, tiles, preferred_element_type=jnp.float32)
    right_gram = jnp.einsum("rki,rkj->ij", tiles, tiles, preferred_element_type=jnp.float32)
    mean_tile = (jnp.sum(tiles.astype(jnp.float32), axis=0) / replicas).astype(jnp.bfloat16)
    identity = jnp.eye(TILE, dtype=jnp.float32)
    stats = jnp.stack([left_gram, right_gram]) / (replicas * TILE) + damping * identity
    roots = inverse_roots(stats)
    half = jnp.dot(roots[0], mean_tile, preferred_element_type=jnp.float32).astype(jnp.bfloat16)
    tile = jnp.dot(half, roots[1], preferred_element_type=jnp.float32).astype(jnp.bfloat16)
    halves = tile.reshape(CORES, rows, TILE)
    outgoing = jnp.broadcast_to(halves[None], (replicas, CORES, rows, TILE)).reshape(group, rows, TILE)
    gathered = lax.all_to_all(outgoing, ("rep", "core"), split_axis=0, concat_axis=0, tiled=True)
    return gathered.transpose(1, 0, 2).reshape(rows, group * TILE)


def solution(mesh):
    shape = mesh.devices.shape
    split = Mesh(mesh.devices.reshape(shape[0], shape[1] // CORES, CORES), ("rep", "row", "core"))
    return jax.shard_map(
        local,
        mesh=split,
        in_specs=(P("rep", None, ("row", "core"), None), P("rep")),
        out_specs=P(("row", "core"), None),
        check_vma=False,
    )
```

```python
import jax
import jax.numpy as jnp
from jax import lax
from jax.experimental import pallas as pl
from jax.experimental.pallas import tpu as pltpu
from jax.sharding import Mesh, PartitionSpec as P

TILE = 512
HALF = 256
NS_ITERS = 5
CORES = 2
REPLICAS = 8
RING = 4
PAIR = 2
GROUP = REPLICAS * CORES
AXES = ("y", "z", "core")

damping = 0.001


def place(y, z, core):
    return (y * PAIR + z) * CORES + core


def shift(block, dy, dz, dc):
    pairs = [
        (place(y, z, c), place((y + dy) % RING, (z + dz) % PAIR, (c + dc) % CORES))
        for y in range(RING)
        for z in range(PAIR)
        for c in range(CORES)
    ]
    return lax.ppermute(block, AXES, pairs)


def dot(left_side, right_side, contract=((1,), (0,))):
    return lax.dot_general(
        left_side, right_side, (contract, ((), ())), preferred_element_type=jnp.float32
    )


def pick_kernel(snap_ref, deltas_ref, out_ref, sems):
    snap = snap_ref[0]
    copies = [
        pltpu.make_async_copy(
            deltas_ref.at[snap, :, pl.ds(k * TILE, TILE)], out_ref.at[k], sems.at[k]
        )
        for k in range(GROUP)
    ]
    for copy in copies:
        copy.start()
    for copy in copies:
        copy.wait()


def pick(snap, deltas):
    return pl.pallas_call(
        pick_kernel,
        out_shape=jax.ShapeDtypeStruct((GROUP, HALF, TILE), jnp.bfloat16),
        in_specs=[pl.BlockSpec(memory_space=pltpu.SMEM), pl.BlockSpec(memory_space=pl.ANY)],
        out_specs=pl.BlockSpec(memory_space=pl.ANY),
        scratch_shapes=[pltpu.SemaphoreType.DMA((GROUP,))],
        name="pick",
    )(snap, deltas)


def tile_kernel(position_ref, recv_ref, own_ref, other_ref, tiles, gram, factor, current, iterate, sems):
    core = position_ref[0] % CORES
    copies = []
    for r in range(REPLICAS):
        for h in range(CORES):
            source = CORES * r + (core if h == 0 else 1 - core)
            copy = pltpu.make_async_copy(
                recv_ref.at[source], tiles.at[r, pl.ds(h * HALF, HALF)], sems.at[r, h]
            )
            copy.start()
            copies.append(copy)
    for r in range(REPLICAS):
        for h in range(CORES):
            copies[CORES * r + h].wait()
        block = tiles[r]
        left, right = dot(block, block, ((1,), (1,))), dot(block, block, ((0,), (0,)))
        gram[0] = left if r == 0 else gram[0] + left
        gram[1] = right if r == 0 else gram[1] + right
    diagonal = lax.broadcasted_iota(jnp.int32, (TILE, TILE), 0) == lax.broadcasted_iota(
        jnp.int32, (TILE, TILE), 1
    )

    def set_current(side, value):
        current[side] = value.astype(jnp.bfloat16)
        factor[side] = jnp.where(diagonal, 1.25 - 0.25 * value, -0.25 * value).astype(jnp.bfloat16)

    scale = []
    for side in range(2):
        stat = gram[side] * (1.0 / (REPLICAS * TILE)) + jnp.where(diagonal, damping, 0.0)
        inverse_norm = lax.rsqrt(jnp.full((1, 1), jnp.sum(stat * stat)))
        scale.append(jnp.sqrt(jnp.sqrt(inverse_norm)))
        set_current(side, stat * inverse_norm)
    for step in range(NS_ITERS):
        last = step + 1 == NS_ITERS
        if not last:
            squares = [dot(factor[s], factor[s]).astype(jnp.bfloat16) for s in range(2)]
        for s in range(2):
            if step == 0:
                iterate[s] = factor[s]
            else:
                product = dot(iterate[s], factor[s])
                iterate[s] = (product * scale[s] if last else product).astype(jnp.bfloat16)
        if not last:
            fourths = [dot(square, square).astype(jnp.bfloat16) for square in squares]
            for s in range(2):
                set_current(s, dot(fourths[s], current[s]))
    total = tiles[0].astype(jnp.float32)
    for r in range(1, REPLICAS):
        total += tiles[r].astype(jnp.float32)
    mean = (total * (1.0 / REPLICAS)).astype(jnp.bfloat16)
    half = dot(iterate[0], mean).astype(jnp.bfloat16)
    result = dot(half, iterate[1]).astype(jnp.bfloat16)
    own_ref[...] = result[:HALF]
    other_ref[...] = result[HALF:]


def tile_update(position, received):
    square = (2, TILE, TILE)
    return pl.pallas_call(
        tile_kernel,
        out_shape=(jax.ShapeDtypeStruct((HALF, TILE), jnp.bfloat16),) * 2,
        in_specs=[pl.BlockSpec(memory_space=pltpu.SMEM), pl.BlockSpec(memory_space=pl.ANY)],
        out_specs=(pl.BlockSpec(memory_space=pltpu.VMEM),) * 2,
        scratch_shapes=[
            pltpu.VMEM((REPLICAS, TILE, TILE), jnp.bfloat16),
            pltpu.VMEM(square, jnp.float32),
            pltpu.VMEM(square, jnp.bfloat16),
            pltpu.VMEM(square, jnp.bfloat16),
            pltpu.VMEM(square, jnp.bfloat16),
            pltpu.SemaphoreType.DMA((REPLICAS, CORES)),
        ],
        compiler_params=pltpu.CompilerParams(vmem_limit_bytes=32 * 2**20),
        cost_estimate=pl.CostEstimate(
            flops=50 * 2 * TILE**3, bytes_accessed=REPLICAS * TILE * TILE * 2, transcendentals=0
        ),
        name="roots",
    )(position, received)


def assemble(position, entries):
    count = len(entries)
    pieces = [entry[0] for entry in entries]

    def kernel(position_ref, *refs):
        sources, out_ref, sems = refs[:count], refs[count], refs[count + 1]
        here = position_ref[0]
        y, z, core = here // (PAIR * CORES), (here // CORES) % PAIR, here % CORES
        copies = []
        for k, source in enumerate(sources):
            _, dy, dz, dc, row = entries[k]
            tile = place((y + RING - dy) % RING, (z + PAIR - dz) % PAIR, (core + CORES - dc) % CORES)
            column = pl.multiple_of(tile * TILE, TILE)
            target = out_ref.at[pl.ds(row, source.shape[0]), pl.ds(column, TILE)]
            copies.append(pltpu.make_async_copy(source, target, sems.at[k]))
        for copy in copies:
            copy.start()
        for copy in copies:
            copy.wait()

    return pl.pallas_call(
        kernel,
        out_shape=jax.ShapeDtypeStruct((HALF, GROUP * TILE), jnp.bfloat16),
        in_specs=[pl.BlockSpec(memory_space=pltpu.SMEM)] + [pl.BlockSpec(memory_space=pl.ANY)] * count,
        out_specs=pl.BlockSpec(memory_space=pl.ANY),
        scratch_shapes=[pltpu.SemaphoreType.DMA((count,))],
        name="assemble",
    )(position, *pieces)


def round_ring(block, dz, dc):
    up, down = shift(block, 1, 0, 0), shift(block, 3, 0, 0)
    mid = HALF // 2
    far_up, far_down = shift(up[:mid], 1, 0, 0), shift(down[mid:], 3, 0, 0)
    return [
        (up, 1, dz, dc, 0),
        (down, 3, dz, dc, 0),
        (far_up, 2, dz, dc, 0),
        (far_down, 2, dz, dc, mid),
    ]


def share(own, other, position):
    swapped = shift(other, 0, 0, 1)
    beside = shift(own, 0, 1, 0)
    second = [(swapped, 0, 0, 1, 0)] + round_ring(swapped, 0, 1)
    first = [(own, 0, 0, 0, 0)] + round_ring(own, 0, 0)
    third = [(beside, 0, 1, 0, 0)] + round_ring(beside, 1, 0)
    fourth = [(shift(block, 0, 1, 0), dy, 1, dc, row) for block, dy, _, dc, row in second]
    entries = first + second + third + fourth
    return assemble(position, entries)


def local(deltas, staleness):
    position = lax.axis_index(AXES).reshape(1).astype(jnp.int32)
    blocks = pick(staleness, deltas[0])
    received = lax.all_to_all(blocks, AXES, split_axis=0, concat_axis=0, tiled=True)
    own, other = tile_update(position, received)
    return share(own, other, position)


def solution(mesh):
    rows = mesh.devices.shape[1] // CORES
    split = Mesh(mesh.devices.reshape(RING, PAIR, rows, CORES), ("y", "z", "row", "core"))
    return jax.shard_map(
        local,
        mesh=split,
        in_specs=(P(("y", "z"), None, ("row", "core"), None), P(("y", "z"))),
        out_specs=P(("row", "core"), None),
        check_vma=False,
    )
```

```python
import jax
import jax.numpy as jnp
from jax import lax
from jax.experimental import pallas as pl
from jax.experimental.pallas import tpu as pltpu
from jax.sharding import Mesh, PartitionSpec as P

TILE = 512
HALF = 256
NS_ITERS = 5
CORES = 2
REPLICAS = 8
RING = 4
PAIR = 2
GROUP = REPLICAS * CORES
AXES = ("y", "z", "core")

damping = 0.001


def place(y, z, core):
    return (y * PAIR + z) * CORES + core


def shift(block, dy, dz, dc):
    pairs = [
        (place(y, z, c), place((y + dy) % RING, (z + dz) % PAIR, (c + dc) % CORES))
        for y in range(RING)
        for z in range(PAIR)
        for c in range(CORES)
    ]
    return lax.ppermute(block, AXES, pairs)


def dot(left_side, right_side, contract=((1,), (0,))):
    return lax.dot_general(
        left_side, right_side, (contract, ((), ())), preferred_element_type=jnp.float32
    )


def pick_kernel(snap_ref, deltas_ref, out_ref, sems):
    snap = snap_ref[0]
    copies = [
        pltpu.make_async_copy(
            deltas_ref.at[snap, :, pl.ds(k * TILE, TILE)], out_ref.at[k], sems.at[k]
        )
        for k in range(GROUP)
    ]
    for copy in copies:
        copy.start()
    for copy in copies:
        copy.wait()


def pick(snap, deltas):
    return pl.pallas_call(
        pick_kernel,
        out_shape=jax.ShapeDtypeStruct((GROUP, HALF, TILE), jnp.bfloat16),
        in_specs=[pl.BlockSpec(memory_space=pltpu.SMEM), pl.BlockSpec(memory_space=pltpu.HBM)],
        out_specs=pl.BlockSpec(memory_space=pltpu.VMEM),
        scratch_shapes=[pltpu.SemaphoreType.DMA((GROUP,))],
        compiler_params=pltpu.CompilerParams(vmem_limit_bytes=52 * 2**20),
        name="pick",
    )(snap, deltas)


def tile_kernel(position_ref, recv_ref, own_ref, other_ref, tiles, gram, factor, current, iterate, sems):
    core = position_ref[0] % CORES
    copies = []
    for r in range(REPLICAS):
        for h in range(CORES):
            source = CORES * r + (core if h == 0 else 1 - core)
            copy = pltpu.make_async_copy(
                recv_ref.at[source], tiles.at[r, pl.ds(h * HALF, HALF)], sems.at[r, h]
            )
            copy.start()
            copies.append(copy)
    for r in range(REPLICAS):
        for h in range(CORES):
            copies[CORES * r + h].wait()
        block = tiles[r]
        left, right = dot(block, block, ((1,), (1,))), dot(block, block, ((0,), (0,)))
        gram[0] = left if r == 0 else gram[0] + left
        gram[1] = right if r == 0 else gram[1] + right
    diagonal = lax.broadcasted_iota(jnp.int32, (TILE, TILE), 0) == lax.broadcasted_iota(
        jnp.int32, (TILE, TILE), 1
    )

    def set_current(side, value):
        current[side] = value.astype(jnp.bfloat16)
        factor[side] = jnp.where(diagonal, 1.25 - 0.25 * value, -0.25 * value).astype(jnp.bfloat16)

    scale = []
    for side in range(2):
        stat = gram[side] * (1.0 / (REPLICAS * TILE)) + jnp.where(diagonal, damping, 0.0)
        inverse_norm = lax.rsqrt(jnp.full((1, 1), jnp.sum(stat * stat)))
        scale.append(jnp.sqrt(jnp.sqrt(inverse_norm)))
        set_current(side, stat * inverse_norm)
    for step in range(NS_ITERS):
        last = step + 1 == NS_ITERS
        if not last:
            squares = [dot(factor[s], factor[s]).astype(jnp.bfloat16) for s in range(2)]
        for s in range(2):
            if step == 0:
                iterate[s] = factor[s]
            else:
                product = dot(iterate[s], factor[s])
                iterate[s] = (product * scale[s] if last else product).astype(jnp.bfloat16)
        if not last:
            fourths = [dot(square, square).astype(jnp.bfloat16) for square in squares]
            for s in range(2):
                set_current(s, dot(fourths[s], current[s]))
    total = tiles[0].astype(jnp.float32)
    for r in range(1, REPLICAS):
        total += tiles[r].astype(jnp.float32)
    mean = (total * (1.0 / REPLICAS)).astype(jnp.bfloat16)
    half = dot(iterate[0], mean).astype(jnp.bfloat16)
    result = dot(half, iterate[1]).astype(jnp.bfloat16)
    own_ref[...] = result[:HALF]
    other_ref[...] = result[HALF:]


def tile_update(position, received):
    square = (2, TILE, TILE)
    return pl.pallas_call(
        tile_kernel,
        out_shape=(jax.ShapeDtypeStruct((HALF, TILE), jnp.bfloat16),) * 2,
        in_specs=[pl.BlockSpec(memory_space=pltpu.SMEM), pl.BlockSpec(memory_space=pl.ANY)],
        out_specs=(pl.BlockSpec(memory_space=pltpu.VMEM),) * 2,
        scratch_shapes=[
            pltpu.VMEM((REPLICAS, TILE, TILE), jnp.bfloat16),
            pltpu.VMEM(square, jnp.float32),
            pltpu.VMEM(square, jnp.bfloat16),
            pltpu.VMEM(square, jnp.bfloat16),
            pltpu.VMEM(square, jnp.bfloat16),
            pltpu.SemaphoreType.DMA((REPLICAS, CORES)),
        ],
        compiler_params=pltpu.CompilerParams(vmem_limit_bytes=32 * 2**20),
        cost_estimate=pl.CostEstimate(
            flops=50 * 2 * TILE**3, bytes_accessed=REPLICAS * TILE * TILE * 2, transcendentals=0
        ),
        name="roots",
    )(position, received)


def assemble(position, entries):
    count = len(entries)
    pieces = [entry[0] for entry in entries]

    def kernel(position_ref, *refs):
        sources, out_ref, sems = refs[:count], refs[count], refs[count + 1]
        here = position_ref[0]
        y, z, core = here // (PAIR * CORES), (here // CORES) % PAIR, here % CORES
        copies = []
        for k, source in enumerate(sources):
            _, dy, dz, dc, row = entries[k]
            tile = place((y + RING - dy) % RING, (z + PAIR - dz) % PAIR, (core + CORES - dc) % CORES)
            column = pl.multiple_of(tile * TILE, TILE)
            target = out_ref.at[pl.ds(row, source.shape[0]), pl.ds(column, TILE)]
            copies.append(pltpu.make_async_copy(source, target, sems.at[k]))
        for copy in copies:
            copy.start()
        for copy in copies:
            copy.wait()

    return pl.pallas_call(
        kernel,
        out_shape=jax.ShapeDtypeStruct((HALF, GROUP * TILE), jnp.bfloat16),
        in_specs=[pl.BlockSpec(memory_space=pltpu.SMEM)] + [pl.BlockSpec(memory_space=pltpu.VMEM)] * count,
        out_specs=pl.BlockSpec(memory_space=pl.ANY),
        scratch_shapes=[pltpu.SemaphoreType.DMA((count,))],
        compiler_params=pltpu.CompilerParams(vmem_limit_bytes=16 * 2**20),
        name="assemble",
    )(position, *pieces)


def round_ring(block, dz, dc):
    up, down = shift(block, 1, 0, 0), shift(block, 3, 0, 0)
    mid = HALF // 2
    far_up, far_down = shift(up[:mid], 1, 0, 0), shift(down[mid:], 3, 0, 0)
    return [
        (up, 1, dz, dc, 0),
        (down, 3, dz, dc, 0),
        (far_up, 2, dz, dc, 0),
        (far_down, 2, dz, dc, mid),
    ]


def share(own, other, position):
    swapped = shift(other, 0, 0, 1)
    beside = shift(own, 0, 1, 0)
    second = [(swapped, 0, 0, 1, 0)] + round_ring(swapped, 0, 1)
    first = [(own, 0, 0, 0, 0)] + round_ring(own, 0, 0)
    third = [(beside, 0, 1, 0, 0)] + round_ring(beside, 1, 0)
    fourth = [(shift(block, 0, 1, 0), dy, 1, dc, row) for block, dy, _, dc, row in second]
    entries = first + second + third + fourth
    return assemble(position, entries)


def local(deltas, staleness):
    position = lax.axis_index(AXES).reshape(1).astype(jnp.int32)
    blocks = pick(staleness, deltas[0])
    received = lax.all_to_all(blocks, AXES, split_axis=0, concat_axis=0, tiled=True)
    own, other = tile_update(position, received)
    return share(own, other, position)


def solution(mesh):
    rows = mesh.devices.shape[1] // CORES
    split = Mesh(mesh.devices.reshape(RING, PAIR, rows, CORES), ("y", "z", "row", "core"))
    return jax.shard_map(
        local,
        mesh=split,
        in_specs=(P(("y", "z"), None, ("row", "core"), None), P(("y", "z"))),
        out_specs=P(("row", "core"), None),
        check_vma=False,
    )
```
